32 devices in a mesh: ctx: 8 (over y, x, core), tp: 4 (over z).
Axes of the slice: x: 2, y: 2, z: 4, core: 2. Of those that a mesh axis runs over, the one named last changes fastest.
Arguments:
- tokens: bfloat16 [4096, 4096], P('ctx'), may hold values from -48 to 48
- w_query: bfloat16 [4096, 4096], P(None, 'tp'), may hold values from -0.09375 to 0.09375
- w_key: bfloat16 [4096, 4096], P(None, 'tp'), may hold values from -0.09375 to 0.09375
- w_value: bfloat16 [4096, 4096], P(None, 'tp'), may hold values from -0.09375 to 0.09375
- w_out: bfloat16 [4096, 4096], P('tp'), may hold values from -0.09375 to 0.09375
- block_doc: int32 [64], replicated, may hold values from 0 to 1, never falling along the last dimension, each value on 1 to 56 neighbouring positions
- grad_out: bfloat16 [4096, 4096], P('ctx', 'tp'), may hold values from -6 to 6
Outputs:
- output: bfloat16 [4096, 4096], P('ctx', 'tp')
- grad_tokens: bfloat16 [4096, 4096], P('ctx', 'tp')
- grad_query_weight: float32 [4096, 4096], P('ctx', 'tp')
- grad_key_weight: float32 [4096, 4096], P('ctx', 'tp')
- grad_value_weight: float32 [4096, 4096], P('ctx', 'tp')
- grad_out_weight: float32 [4096, 4096], P('tp', 'ctx')
The draws below stay inside these ranges and needn't reach their ends.
Inputs may be any that keep to these rules, and one draw needn't show every extreme that they name: block_doc never falls along the blocks; each document covers 1 to 56 consecutive blocks.
All inputs are finite; a program needn't handle non-finite values.
Results may differ from the reference program's by a relative error of at most 0.024.
The reference program's roundings to bfloat16 on the way count: a program that leaves them out, or rounds other values in their place, can miss the bound.
Values may be sent and summed in bfloat16 or wider, within the bound.
A program may use at most 192 MiB of HBM per device.

```python
import math
import jax
import jax.numpy as jnp
import numpy as np
from jax import lax

D = 4096
HEADS = 32
HDIM = 128
BLOCK = 64
SEQ = 4096
NBLK = 64
N_CTX = 8


def draw_tokens(key, part):
    normal_part = jnp.clip(jax.random.normal(key, (SEQ, D), jnp.float32), -6.0, 6.0)
    return normal_part.astype(jnp.bfloat16)


def level_of(own_key, shape, shards, least, top_value):
    def one(axis_at, shards_of):
        draws = jax.random.uniform(jax.random.fold_in(jax.random.fold_in(own_key, 6), axis_at), (shards_of,), jnp.float32, least / len(shards), top_value / len(shards))
        return jnp.repeat(jnp.exp(draws), shape[axis_at] // shards_of).reshape((-1,) + (1,) * (len(shape) - axis_at - 1))

    gain = one(*shards[0])
    for cut in shards[1:]:
        gain = gain * one(*cut)
    return gain


def profile(number_of, total, reach, lean):
    loads = [(1 << 20) // math.isqrt(standing ** lean) + 1 for standing in range(2, number_of + 1)]
    spare, given = total - reach - (number_of - 1), [1] * (number_of - 1)
    while spare > 0:
        candidates = [i for i in range(number_of - 1) if given[i] < reach]
        mass, budget = sum([loads[i] for i in candidates]), spare
        for i in candidates:
            extra = min(reach - given[i], max(1, budget * loads[i] // mass), spare)
            given[i] = given[i] + extra
            spare = spare - extra
    return np.array([reach] + given)


def ragged(own_key, number_of, total, reach, slope):
    if number_of == 2:
        one = jax.random.randint(own_key, (), max(1, total - reach), min(reach, total - 1) + 1)
        return jnp.stack([one, total - one])
    lengths = jnp.asarray(profile(number_of, total, reach, slope), jnp.int32)
    pairs = (number_of - 1) // 2
    giver, receiver = lengths[1:1 + 2 * pairs:2], lengths[2:2 + 2 * pairs:2]
    margin = jnp.minimum(giver - 1, reach - receiver)
    moved = jax.random.randint(jax.random.fold_in(own_key, 1), (pairs,), 0, 1 << 20) % (margin + 1)
    lengths = lengths.at[1:1 + 2 * pairs:2].set(giver - moved).at[2:2 + 2 * pairs:2].set(receiver + moved)
    return lengths[jax.random.permutation(jax.random.fold_in(own_key, 2), number_of)]


def bell_draw(key, shape, spread, limit, split=(), kind=jnp.bfloat16):
    loudness = level_of(key, shape, split, -0.22, 0.18) if split else 1.0
    entries = jax.random.normal(key, shape, jnp.float32) * spread * loudness
    return jnp.minimum(jnp.maximum(entries, -limit), limit).astype(kind)


def setup_inputs(seed: int = 0) -> dict:
    seeds = jax.random.split(jax.random.key(seed), 8)
    tokens = draw_tokens(jax.random.fold_in(seeds[7], 71), 0)
    w_query = bell_draw(seeds[1], (D, D), D ** -0.5, 0.09375, ((1, 4),))
    w_key = bell_draw(seeds[2], (D, D), D ** -0.5, 0.09375, ((1, 4),))
    w_value = bell_draw(seeds[3], (D, D), D ** -0.5, 0.09375, ((1, 4),))
    w_out = bell_draw(seeds[4], (D, D), D ** -0.5, 0.09375, ((0, 4),))
    block_doc = jnp.searchsorted(jnp.cumsum(ragged(seeds[5], 2, NBLK, NBLK - NBLK // 8, 1)), jnp.arange(NBLK), side="right").astype(jnp.int32)
    grad_out = bell_draw(seeds[6], (SEQ, D), 1.0, 6.0, ((0, 8), (1, 4)))
    return {"tokens": tokens, "w_query": w_query, "w_key": w_key, "w_value": w_value, "w_out": w_out, "block_doc": block_doc, "grad_out": grad_out}


big_negative = -1e+30

def elementwise_product(pattern, left_side, right_side):
    left_side, right_side = lax.optimization_barrier((left_side, right_side))
    return jnp.einsum(pattern, left_side.astype(jnp.float32), right_side.astype(jnp.float32), precision=lax.Precision.HIGHEST)

def attend(query_row_matrix, key_row_matrix, value_row_matrix, summary_key, summary_value, allowed, causal, score_scale_factor):
    near_scores = elementwise_product('nqhd,nkhd->nhqk', query_row_matrix, key_row_matrix) * score_scale_factor
    near_scores = jnp.where(causal[None, None], near_scores, big_negative)
    distant_score_matrix = elementwise_product('yzxo,lxo->yzxl', query_row_matrix, summary_key) * score_scale_factor
    distant_score_matrix = jnp.where(allowed[:, None, None, :], distant_score_matrix, big_negative)
    row_top = jnp.maximum(jnp.transpose(lax.optimization_barrier(jnp.max(near_scores, axis=3)), (0, 2, 1)), lax.optimization_barrier(jnp.max(distant_score_matrix, axis=3)))
    near_exp = jnp.exp(near_scores - jnp.transpose(row_top, (0, 2, 1))[..., None])
    far_exp = jnp.exp(distant_score_matrix - row_top[..., None])
    denom_sum = jnp.transpose(lax.optimization_barrier(jnp.sum(near_exp, axis=3)), (0, 2, 1)) + lax.optimization_barrier(jnp.sum(far_exp, axis=3))
    local_weight = (near_exp / jnp.transpose(denom_sum, (0, 2, 1))[..., None]).astype(jnp.bfloat16)
    distant_weight = (far_exp / denom_sum[..., None]).astype(jnp.bfloat16)
    combined_output = elementwise_product('jvyb,jbvo->jyvo', local_weight, value_row_matrix) + elementwise_product('gtuv,vuk->gtuk', distant_weight, summary_value)
    return (combined_output.astype(jnp.bfloat16), local_weight, distant_weight)

def attend_back(query_row_matrix, key_row_matrix, value_row_matrix, summary_key, summary_value, combined_output, local_weight, distant_weight, incoming_gradient, score_scale_factor):
    pair = lax.optimization_barrier((combined_output, incoming_gradient))
    row_delta = lax.optimization_barrier(jnp.sum(pair[0].astype(jnp.float32) * pair[1].astype(jnp.float32), axis=3))
    near_d = elementwise_product('nqhd,nkhd->nhqk', incoming_gradient, value_row_matrix)
    distant_gradient_term = elementwise_product('yzxo,lxo->yzxl', incoming_gradient, summary_value)
    weights = lax.optimization_barrier((local_weight, distant_weight))
    local_score_sum = (weights[0].astype(jnp.float32) * (near_d - jnp.transpose(row_delta, (0, 2, 1))[..., None])).astype(jnp.bfloat16)
    distant_score_sum = (weights[1].astype(jnp.float32) * (distant_gradient_term - row_delta[..., None])).astype(jnp.bfloat16)
    query_gradient = (elementwise_product('jvyb,jbvo->jyvo', local_score_sum, key_row_matrix) + elementwise_product('gtuv,vuk->gtuk', distant_score_sum, summary_key)) * score_scale_factor
    d_key = elementwise_product('nhqk,nqhd->nkhd', local_score_sum, query_row_matrix) * score_scale_factor
    d_value = elementwise_product('nhqk,nqhd->nkhd', local_weight, incoming_gradient)
    summary_key_gradient = elementwise_product('agwi,agwu->iwu', distant_score_sum, query_row_matrix) * score_scale_factor
    summary_value_gradient = elementwise_product('agwi,agwu->iwu', distant_weight, incoming_gradient)
    return (query_gradient, d_key, d_value, summary_key_gradient, summary_value_gradient)

def shard_sum(left_side, right_side):
    shard_rows = left_side.shape[0] // N_CTX

    def add_shard(shard_index, running):
        begin = (shard_index * shard_rows).astype(jnp.int32)
        left_part = lax.dynamic_slice_in_dim(left_side, begin, shard_rows, 0)
        right_part = lax.dynamic_slice_in_dim(right_side, begin, shard_rows, 0)
        term_rows = lax.dot_general(left_part, right_part, (((0,), (0,)), ((), ())), preferred_element_type=jnp.float32)
        term_rows = lax.optimization_barrier(term_rows.astype(jnp.bfloat16))
        return running + term_rows.astype(jnp.float32)
    start_value = jnp.zeros((left_side.shape[1], right_side.shape[1]), jnp.float32)
    return lax.fori_loop(0, N_CTX, add_shard, start_value)

def back_project(grad_rows, weight):
    return lax.dot_general(grad_rows, weight, (((1,), (1,)), ((), ())), preferred_element_type=jnp.float32)

def reference(tokens, w_query, w_key, w_value, w_out, block_doc, grad_out):
    score_scale_factor = 1.0 / math.sqrt(HDIM)
    tok_rows = tokens.shape[0]
    blocks = tok_rows // BLOCK
    block_shape = (blocks, BLOCK, HEADS, HDIM)

    def project(weight):
        return jnp.dot(tokens, weight, preferred_element_type=jnp.float32).astype(jnp.bfloat16)
    query_row_matrix = project(w_query).reshape(block_shape)
    key_row_matrix = project(w_key).reshape(block_shape)
    value_row_matrix = project(w_value).reshape(block_shape)
    summary_key = key_row_matrix[:, BLOCK - 1]
    summary_value = value_row_matrix[:, BLOCK - 1]
    block_ids = jnp.arange(blocks, dtype=jnp.int32)
    allowed = (block_ids[None, :] < block_ids[:, None]) & (block_doc[None, :] == block_doc[:, None])
    positions = jnp.arange(BLOCK, dtype=jnp.int32)
    causal = positions[None, :] <= positions[:, None]
    combined_output, local_weight, distant_weight = attend(query_row_matrix, key_row_matrix, value_row_matrix, summary_key, summary_value, allowed, causal, score_scale_factor)
    attn = combined_output.reshape(tok_rows, D)
    output = (tokens.astype(jnp.float32) + jnp.dot(attn, w_out, preferred_element_type=jnp.float32)).astype(jnp.bfloat16)
    d_attn = back_project(grad_out, w_out).astype(jnp.bfloat16)
    grads = attend_back(query_row_matrix, key_row_matrix, value_row_matrix, summary_key, summary_value, combined_output, local_weight, distant_weight, d_attn.reshape(block_shape), score_scale_factor)
    query_gradient, d_key, d_value, summary_key_gradient, summary_value_gradient = grads
    query_gradient = query_gradient.astype(jnp.bfloat16).reshape(tok_rows, D)
    d_key = d_key.at[:, BLOCK - 1].add(summary_key_gradient).astype(jnp.bfloat16).reshape(tok_rows, D)
    d_value = d_value.at[:, BLOCK - 1].add(summary_value_gradient).astype(jnp.bfloat16).reshape(tok_rows, D)
    grad_tokens = grad_out.astype(jnp.float32) + back_project(query_gradient, w_query) + back_project(d_key, w_key) + back_project(d_value, w_value)
    grad_tokens = grad_tokens.astype(jnp.bfloat16)
    return (output, grad_tokens, shard_sum(tokens, query_gradient), shard_sum(tokens, d_key), shard_sum(tokens, d_value), shard_sum(attn, grad_out))
```

```python
import functools
import math

import jax
import jax.numpy as jnp
from jax import lax
from jax.experimental import pallas as pl
from jax.experimental.pallas import tpu as pltpu
from jax.sharding import PartitionSpec as P

HDIM = 128
BLOCK = 64
HALF = 128

MESH = pl.DeviceIdType.MESH

big_negative = -1e30


def elementwise_product(pattern, left_side, right_side):
    return jnp.einsum(pattern, left_side, right_side, preferred_element_type=jnp.float32)


def attend(
    query_row_matrix,
    key_row_matrix,
    value_row_matrix,
    summary_key,
    summary_value,
    allowed,
    causal,
    score_scale_factor,
):
    near_scores = (
        elementwise_product("nqhd,nkhd->nhqk", query_row_matrix, key_row_matrix)
        * score_scale_factor
    )
    near_scores = jnp.where(causal[None, None], near_scores, big_negative)
    distant_score_matrix = (
        elementwise_product("yzxo,lxo->yzxl", query_row_matrix, summary_key) * score_scale_factor
    )
    distant_score_matrix = jnp.where(allowed[:, None, None, :], distant_score_matrix, big_negative)
    row_top = jnp.maximum(
        jnp.transpose(jnp.max(near_scores, axis=3), (0, 2, 1)),
        jnp.max(distant_score_matrix, axis=3),
    )
    near_exp = jnp.exp(near_scores - jnp.transpose(row_top, (0, 2, 1))[..., None])
    far_exp = jnp.exp(distant_score_matrix - row_top[..., None])
    denom_sum = jnp.transpose(jnp.sum(near_exp, axis=3), (0, 2, 1)) + jnp.sum(far_exp, axis=3)
    local_weight = (near_exp / jnp.transpose(denom_sum, (0, 2, 1))[..., None]).astype(jnp.bfloat16)
    distant_weight = (far_exp / denom_sum[..., None]).astype(jnp.bfloat16)
    combined_output = elementwise_product(
        "jvyb,jbvo->jyvo", local_weight, value_row_matrix
    ) + elementwise_product("gtuv,vuk->gtuk", distant_weight, summary_value)
    return (combined_output.astype(jnp.bfloat16), local_weight, distant_weight)


def attend_back(
    query_row_matrix,
    key_row_matrix,
    value_row_matrix,
    summary_key,
    summary_value,
    combined_output,
    local_weight,
    distant_weight,
    incoming_gradient,
    score_scale_factor,
):
    row_delta = jnp.sum(
        combined_output.astype(jnp.float32) * incoming_gradient.astype(jnp.float32), axis=3
    )
    near_d = elementwise_product("nqhd,nkhd->nhqk", incoming_gradient, value_row_matrix)
    distant_gradient_term = elementwise_product("yzxo,lxo->yzxl", incoming_gradient, summary_value)
    local_score_sum = (
        local_weight.astype(jnp.float32) * (near_d - jnp.transpose(row_delta, (0, 2, 1))[..., None])
    ).astype(jnp.bfloat16)
    distant_score_sum = (
        distant_weight.astype(jnp.float32) * (distant_gradient_term - row_delta[..., None])
    ).astype(jnp.bfloat16)
    query_gradient = (
        elementwise_product("jvyb,jbvo->jyvo", local_score_sum, key_row_matrix)
        + elementwise_product("gtuv,vuk->gtuk", distant_score_sum, summary_key)
    ) * score_scale_factor
    d_key = (
        elementwise_product("nhqk,nqhd->nkhd", local_score_sum, query_row_matrix)
        * score_scale_factor
    )
    d_value = elementwise_product("nhqk,nqhd->nkhd", local_weight, incoming_gradient)
    summary_key_gradient = (
        elementwise_product("agwi,agwu->iwu", distant_score_sum, query_row_matrix)
        * score_scale_factor
    )
    summary_value_gradient = elementwise_product(
        "agwi,agwu->iwu", distant_weight, incoming_gradient
    )
    return (query_gradient, d_key, d_value, summary_key_gradient, summary_value_gradient)


def back_project(grad_rows, weight):
    return lax.dot_general(
        grad_rows, weight, (((1,), (1,)), ((), ())), preferred_element_type=jnp.float32
    )


def column_pieces(partial, axis):
    count = lax.axis_size(axis)
    me = lax.axis_index(axis)
    width = partial.shape[1] // count

    def block(shift):
        return lax.dynamic_slice_in_dim(partial, ((me + shift) % count) * width, width, 1)

    return [block(0)] + [block(shift).astype(jnp.bfloat16) for shift in range(1, count)]


def send_pieces(pieces, axis):
    count = lax.axis_size(axis)
    return [
        lax.ppermute(pieces[shift], axis, [(source, (source + shift) % count) for source in range(count)])
        for shift in range(1, count)
    ]


def tail_kernel(names, cbits, tbits, per, *refs):
    turned_ref, dq_ref, dk_ref, dv_ref, edge_ref, land_ref = refs[:6]
    wq_ref, wk_ref, wv_ref, gout_ref, out_ref, tok_ref = refs[6:12]
    scratch = list(refs[12:])
    grad_ref, weight_buf, total_ref, landed_ref = scratch[:4]
    sent, landed = scratch[4 : 4 + cbits], scratch[4 + cbits : 4 + 2 * cbits]
    scratch = scratch[4 + 2 * cbits :]
    tsent, tlanded = scratch[:tbits], scratch[tbits : 2 * tbits]
    load_sem, weight_sem, land_send, land_recv, send_sem, recv_sem, tsend, trecv = scratch[
        2 * tbits :
    ]
    axis, other_axis = names
    count, tiles, slots = 1 << cbits, landed[0].shape[0], sent[0].shape[0]
    rows = out_ref.shape[1]
    length, width = tok_ref.shape
    sub_width = weight_buf.shape[2]
    subs = width // sub_width
    edge_rows = edge_ref.shape[1]
    me, other_me = lax.axis_index(axis), lax.axis_index(other_axis)
    digit = [(me // (1 << b)) % 2 for b in range(cbits)]
    partner = [me + (1 - 2 * digit[b]) * (1 << b) for b in range(cbits)]
    tdigit = [(other_me // (1 << b)) % 2 for b in range(tbits)]
    tpartner = [other_me + (1 - 2 * tdigit[b]) * (1 << b) for b in range(tbits)]
    rest = list(range(1, cbits))
    orders = ([0] + rest, [0] + rest[::-1])

    loads = [
        pltpu.make_async_copy(ref, grad_ref.at[w], load_sem.at[w])
        for w, ref in enumerate((dq_ref, dk_ref, dv_ref))
    ]
    for load in loads:
        load.start()

    barrier = pltpu.get_barrier_semaphore()
    for shift in range(1, count):
        pl.semaphore_signal(
            barrier, inc=1, device_id={axis: (me + shift) % count}, device_id_type=MESH
        )
    for b in range(tbits):
        pl.semaphore_signal(
            barrier, inc=1, device_id={other_axis: tpartner[b]}, device_id_type=MESH
        )
    pl.semaphore_wait(barrier, count - 1 + tbits)

    def land_copy(shift):
        peer = (me + shift) % count
        return pltpu.make_async_remote_copy(
            src_ref=land_ref.at[pl.ds(pl.multiple_of(peer * edge_rows, edge_rows), edge_rows), :],
            dst_ref=landed_ref.at[shift - 1],
            send_sem=land_send.at[shift - 1],
            recv_sem=land_recv.at[shift - 1],
            device_id={axis: peer},
            device_id_type=MESH,
        )

    for shift in range(1, count):
        land_copy(shift).start()

    def copy(tile, half, stage):
        return pltpu.make_async_remote_copy(
            src_ref=sent[stage].at[tile % slots, half],
            dst_ref=landed[stage].at[tile, half],
            send_sem=send_sem.at[stage, tile, half],
            recv_sem=recv_sem.at[stage, tile, half],
            device_id={axis: partner[orders[half][stage]]},
            device_id_type=MESH,
        )

    def tcopy(stage, at):
        return pltpu.make_async_remote_copy(
            src_ref=tsent[stage].at[at],
            dst_ref=tlanded[stage].at[at],
            send_sem=tsend.at[stage, at],
            recv_sem=trecv.at[stage, at],
            device_id={other_axis: tpartner[stage]},
            device_id_type=MESH,
        )

    def product(row_block, tile, half):
        which = tile // per
        start = pl.multiple_of((tile % per) * 2 * HALF + half * HALF, HALF)
        left = turned_ref[pl.ds(pl.multiple_of(row_block * rows, rows), rows), :]
        return jnp.dot(
            left, grad_ref[which, :, pl.ds(start, HALF)], preferred_element_type=jnp.float32
        )

    def stage_step(tile, stage):
        for half in (0, 1):
            order = orders[half]
            if stage:
                copy(tile, half, stage - 1).wait_recv()
            if stage < cbits:

                @pl.when(tile >= slots)
                def _():
                    copy(tile - slots, half, stage).wait_send()

            for r in range(1 << max(cbits - 1 - stage, 0)):
                if stage == cbits:
                    row_block = me
                else:
                    b = order[stage]
                    row_block = (1 - digit[b]) * (1 << b)
                    for i in range(stage):
                        row_block += digit[order[i]] * (1 << order[i])
                    for i in range(stage + 1, cbits):
                        row_block += ((r >> (cbits - 1 - i)) & 1) * (1 << order[i])
                value = product(row_block, tile, half)
                for t in range(stage):
                    at = r
                    for i in range(t + 1, min(stage, cbits)):
                        at += digit[order[i]] * (1 << (cbits - 1 - i))
                    if stage < cbits:
                        at += (1 - digit[order[stage]]) * (1 << (cbits - 1 - stage))
                    value += landed[t][tile, half, at].astype(jnp.float32)
                if stage < cbits:
                    sent[stage][tile % slots, half, r] = value.astype(jnp.bfloat16)
                else:
                    start = pl.multiple_of((tile % per) * 2 * HALF + half * HALF, HALF)
                    out_ref[tile // per, :, pl.ds(start, HALF)] = value
            if stage < cbits:
                copy(tile, half, stage).start()

    bases = [0]
    for stage in range(tbits):
        bases.append(bases[-1] + subs * (1 << (tbits - 1 - stage)))
    bases.append(bases[-1] + subs)
    turns = bases[-1]

    def weight_loads(k, stage):
        inside = k - bases[stage]
        r, sub = inside // subs, inside % subs
        if stage == tbits:
            block = other_me
        else:
            block = (1 - tdigit[stage]) * (1 << stage)
            for i in range(stage):
                block += tdigit[i] * (1 << i)
            for i in range(stage + 1, tbits):
                block += ((r // (1 << (tbits - 1 - i))) % 2) * (1 << i)
        start = pl.multiple_of(block * width + sub * sub_width, sub_width)
        return [
            pltpu.make_async_copy(
                ref.at[pl.ds(start, sub_width), :], weight_buf.at[k % 2, w], weight_sem.at[k % 2, w]
            )
            for w, ref in enumerate((wq_ref, wk_ref, wv_ref))
        ]

    def fetch(k):
        for stage in range(tbits + 1):

            @pl.when((k >= bases[stage]) & (k < bases[stage + 1]))
            def _():
                for load in weight_loads(k, stage):
                    load.start()

    def turn(k):
        for load in weight_loads(k, 0):
            load.wait()
        fetch(k + 1)
        value = None
        for w in range(3):
            term = lax.dot_general(
                grad_ref[w],
                weight_buf[k % 2, w],
                (((1,), (1,)), ((), ())),
                preferred_element_type=jnp.float32,
            )
            value = term if value is None else value + term
        total_ref[...] = value
        for stage in range(tbits + 1):

            @pl.when((k >= bases[stage]) & (k < bases[stage + 1]))
            def _():
                inside = k - bases[stage]
                result = total_ref[...]
                for t in range(stage):
                    at = inside // subs
                    for i in range(t + 1, min(stage, tbits)):
                        at += tdigit[i] * (1 << (tbits - 1 - i))
                    if stage < tbits:
                        at += (1 - tdigit[stage]) * (1 << (tbits - 1 - stage))
                    spot = at * subs + inside % subs
                    tcopy(t, spot).wait_recv()
                    result += tlanded[t][spot].astype(jnp.float32)
                if stage < tbits:
                    tsent[stage][inside] = result.astype(jnp.bfloat16)
                    tcopy(stage, inside).start()
                else:
                    start = pl.multiple_of(inside * sub_width, sub_width)
                    mine = gout_ref[:, pl.ds(start, sub_width)].astype(jnp.float32)
                    tok_ref[:, pl.ds(start, sub_width)] = (mine + result).astype(jnp.bfloat16)

    def finish_edges():
        loads[1].wait()
        loads[2].wait()
        for shift in range(1, count):
            land_copy(shift).wait_recv()
        columns = edge_ref.shape[2]
        own = pl.ds(pl.multiple_of(me * edge_rows, edge_rows), edge_rows)
        for p in (0, 1):
            part = slice(p * columns, (p + 1) * columns)
            total = edge_ref[p] + land_ref[own, part]
            for shift in range(1, count):
                total += landed_ref[shift - 1, :, part]
            for j in range(edge_rows):
                chunk = slice((j + 1) * BLOCK - 16, (j + 1) * BLOCK)
                old = grad_ref[1 + p, chunk, :].astype(jnp.float32)
                last = lax.broadcasted_iota(jnp.int32, old.shape, 0) == 15
                new = jnp.where(last, total[j : j + 1, :], old)
                grad_ref[1 + p, chunk, :] = new.astype(jnp.bfloat16)

    fetch(0)
    loads[0].wait()
    lags = [0] + [2 * s - 1 for s in range(1, cbits + 1)]

    def body(i, carry):
        for stage in range(cbits, -1, -1):
            tile = i - lags[stage]

            @pl.when((tile >= 0) & (tile < tiles))
            def _():
                stage_step(tile, stage)

        @pl.when(i == 0)
        def _():
            finish_edges()

        @pl.when((i >= 1) & (i <= turns))
        def _():
            turn(i - 1)

        return carry

    lax.fori_loop(0, max(tiles + lags[cbits], turns + 1), body, 0)
    for tile in range(max(tiles - slots, 0), tiles):
        for half in (0, 1):
            for stage in range(cbits):
                copy(tile, half, stage).wait_send()
    for stage in range(tbits):
        for at in range(tsent[stage].shape[0]):
            tcopy(stage, at).wait_send()
    for shift in range(1, count):
        land_copy(shift).wait_send()


def tail(turned, grads, edges, land, weights, grad_out, names, call):
    axis, other_axis = names
    count, other_count = lax.axis_size(axis), lax.axis_size(other_axis)
    cbits, tbits = count.bit_length() - 1, other_count.bit_length() - 1
    depth, length = turned.shape
    columns = grads[0].shape[1]
    width = grad_out.shape[1]
    rows = depth // count
    per = columns // (2 * HALF)
    tiles = 3 * per
    slots = min(4, tiles)
    sub_width = min(2 * HALF, width)
    subs = width // sub_width
    blocks = [1 << (cbits - 1 - stage) for stage in range(cbits)]
    tblocks = [subs << (tbits - 1 - stage) for stage in range(tbits)]
    edge_rows = edges.shape[1]
    vmem = pl.BlockSpec(memory_space=pltpu.VMEM)
    hbm = pl.BlockSpec(memory_space=pl.ANY)
    dma = pltpu.SemaphoreType.DMA
    return pl.pallas_call(
        functools.partial(tail_kernel, names, cbits, tbits, per),
        out_shape=[
            jax.ShapeDtypeStruct((3, rows, columns), jnp.float32),
            jax.ShapeDtypeStruct((length, width), jnp.bfloat16),
        ],
        in_specs=[vmem, hbm, hbm, hbm, vmem, vmem, hbm, hbm, hbm, vmem],
        out_specs=[vmem, vmem],
        scratch_shapes=[
            pltpu.VMEM((3, length, columns), jnp.bfloat16),
            pltpu.VMEM((2, 3, sub_width, columns), jnp.bfloat16),
            pltpu.VMEM((length, sub_width), jnp.float32),
            pltpu.VMEM((count - 1, edge_rows, 2 * columns), jnp.float32),
        ]
        + [pltpu.VMEM((slots, 2, n, rows, HALF), jnp.bfloat16) for n in blocks]
        + [pltpu.VMEM((tiles, 2, n, rows, HALF), jnp.bfloat16) for n in blocks]
        + [pltpu.VMEM((n, length, sub_width), jnp.bfloat16) for n in tblocks] * 2
        + [dma((3,)), dma((2, 3)), dma((count - 1,)), dma((count - 1,))]
        + [dma((cbits, tiles, 2)), dma((cbits, tiles, 2))]
        + [dma((tbits, tblocks[0])), dma((tbits, tblocks[0]))],
        compiler_params=pltpu.CompilerParams(
            collective_id=call, has_side_effects=True, vmem_limit_bytes=63 * 1024 * 1024
        ),
        cost_estimate=pl.CostEstimate(
            flops=12 * depth * length * columns,
            bytes_accessed=2 * (depth * length + 3 * length * columns + 3 * depth * columns),
            transcendentals=0,
        ),
        name="tail",
    )(turned, *grads, edges, land, *weights, grad_out)


def per_device(tokens, w_query, w_key, w_value, w_out, block_doc, grad_out):
    score_scale_factor = 1.0 / math.sqrt(HDIM)
    tok_rows = tokens.shape[0]
    col_count = w_query.shape[1]
    blocks = tok_rows // BLOCK
    head_count = col_count // HDIM
    block_shape = (blocks, BLOCK, head_count, HDIM)
    upstream_full = lax.all_gather(grad_out, "tp", axis=1, tiled=True)

    def project(weight):
        return jnp.dot(tokens, weight, preferred_element_type=jnp.float32).astype(jnp.bfloat16)

    query_row_matrix = project(w_query).reshape(block_shape)
    key_row_matrix = project(w_key).reshape(block_shape)
    value_row_matrix = project(w_value).reshape(block_shape)
    own_key = key_row_matrix[:, BLOCK - 1].reshape(blocks, col_count)
    own_value = value_row_matrix[:, BLOCK - 1].reshape(blocks, col_count)
    summary = lax.all_gather(
        jnp.concatenate([own_key, own_value], axis=1), "ctx", axis=0, tiled=True
    )
    summary_key, summary_value = summary[:, :col_count], summary[:, col_count:]
    total_blocks = summary_key.shape[0]
    summary_key = summary_key.reshape(total_blocks, head_count, HDIM)
    summary_value = summary_value.reshape(total_blocks, head_count, HDIM)
    first_block = lax.axis_index("ctx") * blocks
    query_ids = first_block + jnp.arange(blocks, dtype=jnp.int32)
    own_doc = lax.dynamic_slice_in_dim(block_doc, first_block, blocks, 0)
    block_ids = jnp.arange(total_blocks, dtype=jnp.int32)
    allowed = (block_ids[None, :] < query_ids[:, None]) & (block_doc[None, :] == own_doc[:, None])
    positions = jnp.arange(BLOCK, dtype=jnp.int32)
    causal = positions[None, :] <= positions[:, None]
    combined_output, local_weight, distant_weight = attend(
        query_row_matrix,
        key_row_matrix,
        value_row_matrix,
        summary_key,
        summary_value,
        allowed,
        causal,
        score_scale_factor,
    )
    attn = combined_output.reshape(tok_rows, col_count)
    partial_value = jnp.dot(attn, w_out, preferred_element_type=jnp.float32)
    turned = tokens.T
    pieces = column_pieces(partial_value, "tp")
    upstream_full, pieces, turned = lax.optimization_barrier((upstream_full, pieces, turned))
    moved = send_pieces(pieces, "tp")
    d_attn = back_project(upstream_full, w_out).astype(jnp.bfloat16)
    grads = attend_back(
        query_row_matrix,
        key_row_matrix,
        value_row_matrix,
        summary_key,
        summary_value,
        combined_output,
        local_weight,
        distant_weight,
        d_attn.reshape(block_shape),
        score_scale_factor,
    )
    query_gradient, d_key, d_value, summary_key_gradient, summary_value_gradient = grads
    flat_key = summary_key_gradient.reshape(total_blocks, col_count)
    flat_value = summary_value_gradient.reshape(total_blocks, col_count)
    out_term = lax.dot_general(
        attn, upstream_full, (((0,), (0,)), ((), ())), preferred_element_type=jnp.float32
    )
    grad_out_weight = lax.psum_scatter(
        out_term.astype(jnp.bfloat16), "ctx", scatter_dimension=1, tiled=True
    ).astype(jnp.float32)
    edges = jnp.stack(
        [d_key[:, BLOCK - 1].reshape(blocks, col_count), d_value[:, BLOCK - 1].reshape(blocks, col_count)]
    )
    rows_of = [
        part.astype(jnp.bfloat16).reshape(tok_rows, col_count)
        for part in (query_gradient, d_key, d_value)
    ]
    joined, grad_tokens = tail(
        turned,
        rows_of,
        edges,
        jnp.concatenate([flat_key, flat_value], axis=1),
        (w_query, w_key, w_value),
        grad_out,
        ("ctx", "tp"),
        0,
    )
    joined, moved = lax.optimization_barrier((joined, moved))
    shard_width = grad_out.shape[1]
    summed = lax.dynamic_slice_in_dim(tokens, lax.axis_index("tp") * shard_width, shard_width, 1)
    summed = summed.astype(jnp.float32) + pieces[0]
    for piece in moved:
        summed = summed + piece.astype(jnp.float32)
    output = summed.astype(jnp.bfloat16)
    return (output, grad_tokens, joined[0], joined[1], joined[2], grad_out_weight)


def solution(mesh):
    in_specs = (
        P("ctx", None),
        P(None, "tp"),
        P(None, "tp"),
        P(None, "tp"),
        P("tp", None),
        P(),
        P("ctx", "tp"),
    )
    out_specs = (
        P("ctx", "tp"),
        P("ctx", "tp"),
        P("ctx", "tp"),
        P("ctx", "tp"),
        P("ctx", "tp"),
        P("tp", "ctx"),
    )
    return jax.shard_map(
        per_device, mesh=mesh, in_specs=in_specs, out_specs=out_specs, check_vma=False
    )
```

```python
import functools
import math

import jax
import jax.numpy as jnp
from jax import lax
from jax.experimental import pallas as pl
from jax.experimental.pallas import tpu as pltpu
from jax.sharding import PartitionSpec as P

HDIM = 128
BLOCK = 64
HALF = 128

MESH = pl.DeviceIdType.MESH

big_negative = -1e30


def elementwise_product(pattern, left_side, right_side):
    return jnp.einsum(pattern, left_side, right_side, preferred_element_type=jnp.float32)


def attend(
    query_row_matrix,
    key_row_matrix,
    value_row_matrix,
    summary_key,
    summary_value,
    allowed,
    causal,
    score_scale_factor,
):
    near_scores = (
        elementwise_product("nqhd,nkhd->nhqk", query_row_matrix, key_row_matrix)
        * score_scale_factor
    )
    near_scores = jnp.where(causal[None, None], near_scores, big_negative)
    distant_score_matrix = (
        elementwise_product("yzxo,lxo->yzxl", query_row_matrix, summary_key) * score_scale_factor
    )
    distant_score_matrix = jnp.where(allowed[:, None, None, :], distant_score_matrix, big_negative)
    row_top = jnp.maximum(
        jnp.transpose(jnp.max(near_scores, axis=3), (0, 2, 1)),
        jnp.max(distant_score_matrix, axis=3),
    )
    near_exp = jnp.exp(near_scores - jnp.transpose(row_top, (0, 2, 1))[..., None])
    far_exp = jnp.exp(distant_score_matrix - row_top[..., None])
    denom_sum = jnp.transpose(jnp.sum(near_exp, axis=3), (0, 2, 1)) + jnp.sum(far_exp, axis=3)
    local_weight = (near_exp / jnp.transpose(denom_sum, (0, 2, 1))[..., None]).astype(jnp.bfloat16)
    distant_weight = (far_exp / denom_sum[..., None]).astype(jnp.bfloat16)
    combined_output = elementwise_product(
        "jvyb,jbvo->jyvo", local_weight, value_row_matrix
    ) + elementwise_product("gtuv,vuk->gtuk", distant_weight, summary_value)
    return combined_output.astype(jnp.bfloat16)


def column_pieces(partial, axis):
    count = lax.axis_size(axis)
    me = lax.axis_index(axis)
    width = partial.shape[1] // count

    def block(shift):
        return lax.dynamic_slice_in_dim(partial, ((me + shift) % count) * width, width, 1)

    return [block(0)] + [block(shift).astype(jnp.bfloat16) for shift in range(1, count)]


def send_pieces(pieces, axis):
    count = lax.axis_size(axis)
    return [
        lax.ppermute(pieces[shift], axis, [(source, (source + shift) % count) for source in range(count)])
        for shift in range(1, count)
    ]


def tail_kernel(names, scale, cbits, tbits, per, *refs):
    up_ref, turned_ref, attn_ref, query_ref, key_ref, value_ref, wout_ref = refs[:7]
    wq_ref, wk_ref, wv_ref, sk_ref, sv_ref, mask_ref, gout_ref, out_ref, tok_ref = refs[7:16]
    scratch = list(refs[16:])
    q_ref, wout_buf, edge_ref, land_ref, head_sem = scratch[:5]
    scratch = scratch[5:]
    left_ref, grad_ref, weight_buf, total_ref, landed_ref = scratch[:5]
    sent, landed = scratch[5 : 5 + cbits], scratch[5 + cbits : 5 + 2 * cbits]
    scratch = scratch[5 + 2 * cbits :]
    tsent, tlanded = scratch[:tbits], scratch[tbits : 2 * tbits]
    load_sem, weight_sem, land_send, land_recv, send_sem, recv_sem, tsend, trecv, free_sem = scratch[
        2 * tbits :
    ]
    axis, other_axis = names
    count, tiles, slots = 1 << cbits, 4 * per, sent[0].shape[0]
    ring = landed[0].shape[0]
    rows = out_ref.shape[1]
    length, width = tok_ref.shape
    sub_width = weight_buf.shape[2]
    subs = width // sub_width
    edge_rows = edge_ref.shape[1]
    me, other_me = lax.axis_index(axis), lax.axis_index(other_axis)
    digit = [(me // (1 << b)) % 2 for b in range(cbits)]
    partner = [me + (1 - 2 * digit[b]) * (1 << b) for b in range(cbits)]
    tdigit = [(other_me // (1 << b)) % 2 for b in range(tbits)]
    tpartner = [other_me + (1 - 2 * tdigit[b]) * (1 << b) for b in range(tbits)]
    rest = list(range(1, cbits))
    orders = ([0] + rest, [0] + rest[::-1])

    moves = (
        (up_ref, left_ref.at[0]),
        (attn_ref, grad_ref.at[0]),
        (query_ref, q_ref),
        (key_ref, grad_ref.at[2]),
        (value_ref, grad_ref.at[3]),
        (turned_ref, left_ref.at[1]),
    )
    loads = [
        pltpu.make_async_copy(source, target, load_sem.at[w])
        for w, (source, target) in enumerate(moves)
    ]
    for load in loads:
        load.start()

    barrier = pltpu.get_barrier_semaphore()
    for shift in range(1, count):
        pl.semaphore_signal(
            barrier, inc=1, device_id={axis: (me + shift) % count}, device_id_type=MESH
        )
    for b in range(tbits):
        pl.semaphore_signal(
            barrier, inc=1, device_id={other_axis: tpartner[b]}, device_id_type=MESH
        )
    pl.semaphore_wait(barrier, count - 1 + tbits)

    def land_copy(shift):
        peer = (me + shift) % count
        return pltpu.make_async_remote_copy(
            src_ref=land_ref.at[:, pl.ds(pl.multiple_of(peer * edge_rows, edge_rows), edge_rows), :],
            dst_ref=landed_ref.at[shift - 1],
            send_sem=land_send.at[shift - 1],
            recv_sem=land_recv.at[shift - 1],
            device_id={axis: peer},
            device_id_type=MESH,
        )

    def place(tile, stage):
        return tile if stage else tile % ring

    def copy(tile, half, stage):
        return pltpu.make_async_remote_copy(
            src_ref=sent[stage].at[tile % slots, half],
            dst_ref=landed[stage].at[place(tile, stage), half],
            send_sem=send_sem.at[stage, tile, half],
            recv_sem=recv_sem.at[stage, tile, half],
            device_id={axis: partner[orders[half][stage]]},
            device_id_type=MESH,
        )

    def tcopy(stage, at):
        return pltpu.make_async_remote_copy(
            src_ref=tsent[stage].at[at],
            dst_ref=tlanded[stage].at[at],
            send_sem=tsend.at[stage, at],
            recv_sem=trecv.at[stage, at],
            device_id={other_axis: tpartner[stage]},
            device_id_type=MESH,
        )

    def product(row_block, tile, half):
        which = tile // per
        start = pl.multiple_of((tile % per) * 2 * HALF + half * HALF, HALF)
        side = jnp.minimum(which, 1)
        left = left_ref[side, pl.ds(pl.multiple_of(row_block * rows, rows), rows), :]
        return jnp.dot(
            left, grad_ref[which, :, pl.ds(start, HALF)], preferred_element_type=jnp.float32
        )

    def first_step(tile):
        @pl.when(tile >= slots)
        def _():
            for half in (0, 1):
                copy(tile - slots, half, 0).wait_send()

        which, spot = tile // per, tile % slots
        start = pl.multiple_of((tile % per) * 2 * HALF, 2 * HALF)
        side = jnp.minimum(which, 1)
        for high in range(1 << (cbits - 1)):
            row_block = (1 - digit[0]) + 2 * high
            left = left_ref[side, pl.ds(pl.multiple_of(row_block * rows, rows), rows), :]
            value = jnp.dot(
                left, grad_ref[which, :, pl.ds(start, 2 * HALF)], preferred_element_type=jnp.float32
            ).astype(jnp.bfloat16)
            for half in (0, 1):
                r = 0
                for i in range(1, cbits):
                    r += ((2 * high >> orders[half][i]) & 1) << (cbits - 1 - i)
                sent[0][spot, half, r] = value[:, half * HALF : (half + 1) * HALF]
        for half in (0, 1):
            copy(tile, half, 0).start()

    def stage_step(tile, stage):
        if stage == 0 and ring < tiles:

            @pl.when(tile >= ring)
            def _():
                pl.semaphore_wait(free_sem, 1)

        if stage == 0:
            first_step(tile)
            return

        for half in (0, 1):
            order = orders[half]
            if stage:
                copy(tile, half, stage - 1).wait_recv()
            if stage < cbits:

                @pl.when(tile >= slots)
                def _():
                    copy(tile - slots, half, stage).wait_send()

            for r in range(1 << max(cbits - 1 - stage, 0)):
                if stage == cbits:
                    row_block = me
                else:
                    b = order[stage]
                    row_block = (1 - digit[b]) * (1 << b)
                    for i in range(stage):
                        row_block += digit[order[i]] * (1 << order[i])
                    for i in range(stage + 1, cbits):
                        row_block += ((r >> (cbits - 1 - i)) & 1) * (1 << order[i])
                value = product(row_block, tile, half)
                for t in range(stage):
                    at = r
                    for i in range(t + 1, min(stage, cbits)):
                        at += digit[order[i]] * (1 << (cbits - 1 - i))
                    if stage < cbits:
                        at += (1 - digit[order[stage]]) * (1 << (cbits - 1 - stage))
                    value += landed[t][place(tile, t), half, at].astype(jnp.float32)
                if stage < cbits:
                    sent[stage][tile % slots, half, r] = value.astype(jnp.bfloat16)
                else:
                    start = pl.multiple_of((tile % per) * 2 * HALF + half * HALF, HALF)
                    out_ref[tile // per, :, pl.ds(start, HALF)] = value
            if stage < cbits:
                copy(tile, half, stage).start()
        if stage == cbits and ring < tiles:

            @pl.when(tile < tiles - ring)
            def _():
                pl.semaphore_signal(
                    free_sem, inc=1, device_id={axis: partner[0]}, device_id_type=MESH
                )

    bases = [0]
    for stage in range(tbits):
        bases.append(bases[-1] + subs * (1 << (tbits - 1 - stage)))
    bases.append(bases[-1] + subs)
    turns = bases[-1]

    def weight_loads(k, stage):
        inside = k - bases[stage]
        r, sub = inside // subs, inside % subs
        if stage == tbits:
            block = other_me
        else:
            block = (1 - tdigit[stage]) * (1 << stage)
            for i in range(stage):
                block += tdigit[i] * (1 << i)
            for i in range(stage + 1, tbits):
                block += ((r // (1 << (tbits - 1 - i))) % 2) * (1 << i)
        start = pl.multiple_of(block * width + sub * sub_width, sub_width)
        return [
            pltpu.make_async_copy(
                ref.at[pl.ds(start, sub_width), :], weight_buf.at[k % 2, w], weight_sem.at[k % 2, w]
            )
            for w, ref in enumerate((wq_ref, wk_ref, wv_ref))
        ]

    def fetch(k):
        for stage in range(tbits + 1):

            @pl.when((k >= bases[stage]) & (k < bases[stage + 1]))
            def _():
                for load in weight_loads(k, stage):
                    load.start()

    def turn(k, stages):
        for load in weight_loads(k, 0):
            load.wait()
        fetch(k + 1)
        value = None
        for w in range(3):
            term = lax.dot_general(
                grad_ref[1 + w],
                weight_buf[k % 2, w],
                (((1,), (1,)), ((), ())),
                preferred_element_type=jnp.float32,
            )
            value = term if value is None else value + term
        total_ref[...] = value
        for stage in stages:

            @pl.when((k >= bases[stage]) & (k < bases[stage + 1]))
            def _():
                inside = k - bases[stage]
                result = total_ref[...]
                for t in range(stage):
                    at = inside // subs
                    for i in range(t + 1, min(stage, tbits)):
                        at += tdigit[i] * (1 << (tbits - 1 - i))
                    if stage < tbits:
                        at += (1 - tdigit[stage]) * (1 << (tbits - 1 - stage))
                    spot = at * subs + inside % subs
                    tcopy(t, spot).wait_recv()
                    result += tlanded[t][spot].astype(jnp.float32)
                if stage < tbits:
                    tsent[stage][inside] = result.astype(jnp.bfloat16)
                    tcopy(stage, inside).start()
                else:
                    start = pl.multiple_of(inside * sub_width, sub_width)
                    mine = gout_ref[:, pl.ds(start, sub_width)].astype(jnp.float32)
                    tok_ref[:, pl.ds(start, sub_width)] = (mine + result).astype(jnp.bfloat16)

    def head_load(h):
        start = pl.multiple_of(h * 2 * HALF, 2 * HALF)
        return pltpu.make_async_copy(
            wout_ref.at[pl.ds(start, 2 * HALF), :], wout_buf, head_sem.at[0]
        )

    def dot(left, right, left_dim, right_dim):
        dims = (((left_dim,), (right_dim,)), ((), ()))
        return lax.dot_general(left, right, dims, preferred_element_type=jnp.float32)

    def attn_grads(h):
        head_load(h).wait()
        columns = pl.ds(pl.multiple_of(h * 2 * HALF, 2 * HALF), 2 * HALF)
        grad_ref[1, :, columns] = dot(wout_buf[...], left_ref[0], 1, 0).T.astype(jnp.bfloat16)

        @pl.when(h + 1 < per)
        def _():
            head_load(h + 1).start()

    def attend_back(h):
        columns = pl.ds(pl.multiple_of(h * HDIM, HDIM), HDIM)
        sk, sv = sk_ref[:, columns], sv_ref[:, columns]
        group = min(2 * BLOCK, length)
        total_blocks = land_ref.shape[1]
        spot = lax.broadcasted_iota(jnp.int32, (group, group), 0)
        other = lax.broadcasted_iota(jnp.int32, (group, group), 1)
        causal = (spot // BLOCK == other // BLOCK) & (other <= spot)
        causal = jnp.where(causal, 1.0, 0.0)
        land_key = jnp.zeros(sk.shape, jnp.float32)
        land_value = jnp.zeros(sk.shape, jnp.float32)
        for g in range(length // group):
            part = slice(g * group, (g + 1) * group)
            q, grad = q_ref[part, columns], grad_ref[1, part, columns]
            keys = jnp.concatenate([grad_ref[2, part, columns], sk], axis=0)
            values = jnp.concatenate([grad_ref[3, part, columns], sv], axis=0)
            inside = jnp.concatenate([causal, mask_ref[part, :]], axis=1) > 0.0
            score = jnp.where(inside, dot(q, keys, 1, 1) * scale, big_negative)
            weight = jnp.exp(score - jnp.max(score, axis=1, keepdims=True))
            weight = weight * (1.0 / jnp.sum(weight, axis=1, keepdims=True))
            weight = weight.astype(jnp.bfloat16)
            attn = grad_ref[0, part, columns].astype(jnp.float32)
            delta = jnp.sum(attn * grad.astype(jnp.float32), axis=1, keepdims=True)
            change = weight.astype(jnp.float32) * (dot(grad, values, 1, 1) - delta)
            change = change.astype(jnp.bfloat16)
            dq = dot(change, keys, 1, 0) * scale
            dk = dot(change, q, 0, 0) * scale
            dv = dot(weight, grad, 0, 0)
            grad_ref[1, part, columns] = dq.astype(jnp.bfloat16)
            grad_ref[2, part, columns] = dk[:group].astype(jnp.bfloat16)
            grad_ref[3, part, columns] = dv[:group].astype(jnp.bfloat16)
            for b in range(group // BLOCK):
                row = slice((b + 1) * BLOCK - 1, (b + 1) * BLOCK)
                at = g * (group // BLOCK) + b
                edge_ref[0, at : at + 1, columns] = dk[row, :]
                edge_ref[1, at : at + 1, columns] = dv[row, :]
            land_key += dk[group:]
            land_value += dv[group:]
        land_ref[0, :, columns] = land_key[:total_blocks]
        land_ref[1, :, columns] = land_value[:total_blocks]

    def finish_edges():
        for shift in range(1, count):
            land_copy(shift).wait_recv()
        own = pl.ds(pl.multiple_of(me * edge_rows, edge_rows), edge_rows)
        for p in (0, 1):
            total = edge_ref[p] + land_ref[p, own, :]
            for shift in range(1, count):
                total += landed_ref[shift - 1, p]
            for j in range(edge_rows):
                chunk = slice((j + 1) * BLOCK - 16, (j + 1) * BLOCK)
                old = grad_ref[2 + p, chunk, :].astype(jnp.float32)
                last = lax.broadcasted_iota(jnp.int32, old.shape, 0) == 15
                new = jnp.where(last, total[j : j + 1, :], old)
                grad_ref[2 + p, chunk, :] = new.astype(jnp.bfloat16)

    fetch(0)
    head_load(0).start()
    for load in loads[:5]:
        load.wait()

    def head_body(e, i):
        attend_back(i * (2 * HALF // HDIM) + e)
        return i

    first = per
    second = first + bases[1] // 2 + 4
    lags = [0] + [2 * s - 1 for s in range(1, cbits + 1)]

    def body(i, carry):
        @pl.when(i == per)
        def _():
            loads[5].wait()

            for shift in range(1, count):
                land_copy(shift).start()

        for stage in range(cbits, -1, -1):
            tile = i - lags[stage]

            @pl.when((tile >= 0) & (tile < tiles))
            def _():
                stage_step(tile, stage)

        @pl.when(i < per)
        def _():
            attn_grads(i)
            lax.fori_loop(0, 2 * HALF // HDIM, head_body, i)

        @pl.when(i == per)
        def _():
            finish_edges()

        @pl.when((i >= first) & (i < first + bases[1] // 2))
        def _():
            turn(2 * (i - first), (0,))
            turn(2 * (i - first) + 1, (0,))

        @pl.when((i >= second) & (i < second + turns - bases[1]))
        def _():
            turn(bases[1] + i - second, range(1, tbits + 1))

        return carry

    lax.fori_loop(0, max(tiles + lags[cbits], second + turns - bases[1]), body, 0)
    for tile in range(max(tiles - slots, 0), tiles):
        for half in (0, 1):
            for stage in range(cbits):
                copy(tile, half, stage).wait_send()
    for stage in range(tbits):
        for at in range(tsent[stage].shape[0]):
            tcopy(stage, at).wait_send()
    for shift in range(1, count):
        land_copy(shift).wait_send()


def tail(upstream, turned, rows_in, weights, summaries, allowed, grad_out, names, scale, call):
    axis, other_axis = names
    count, other_count = lax.axis_size(axis), lax.axis_size(other_axis)
    cbits, tbits = count.bit_length() - 1, other_count.bit_length() - 1
    depth, length = turned.shape
    columns = rows_in[0].shape[1]
    width = grad_out.shape[1]
    rows = depth // count
    per = columns // (2 * HALF)
    tiles = 4 * per
    slots = min(3, tiles)
    ring = min(tiles, 2 * cbits + 2)
    sub_width = min(2 * HALF, width)
    subs = width // sub_width
    blocks = [1 << (cbits - 1 - stage) for stage in range(cbits)]
    tblocks = [subs << (tbits - 1 - stage) for stage in range(tbits)]
    edge_rows = length // BLOCK
    total_blocks = summaries[0].shape[0]
    spare = -total_blocks % HALF
    summaries = [jnp.pad(part, ((0, spare), (0, 0))) for part in summaries]
    mask = jnp.repeat(allowed.astype(jnp.float32), BLOCK, axis=0)
    mask = jnp.pad(mask, ((0, 0), (0, spare)))
    vmem = pl.BlockSpec(memory_space=pltpu.VMEM)
    hbm = pl.BlockSpec(memory_space=pl.ANY)
    dma = pltpu.SemaphoreType.DMA
    return pl.pallas_call(
        functools.partial(tail_kernel, names, scale, cbits, tbits, per),
        out_shape=[
            jax.ShapeDtypeStruct((4, rows, columns), jnp.float32),
            jax.ShapeDtypeStruct((length, width), jnp.bfloat16),
        ],
        in_specs=[hbm] * 10 + [vmem] * 4,
        out_specs=[vmem, vmem],
        scratch_shapes=[
            pltpu.VMEM((length, columns), jnp.bfloat16),
            pltpu.VMEM((2 * HALF, depth), jnp.bfloat16),
            pltpu.VMEM((2, edge_rows, columns), jnp.float32),
            pltpu.VMEM((2, total_blocks, columns), jnp.float32),
            dma((1,)),
            pltpu.VMEM((2, depth, length), jnp.bfloat16),
            pltpu.VMEM((4, length, columns), jnp.bfloat16),
            pltpu.VMEM((2, 3, sub_width, columns), jnp.bfloat16),
            pltpu.VMEM((length, sub_width), jnp.float32),
            pltpu.VMEM((count - 1, 2, edge_rows, columns), jnp.float32),
        ]
        + [pltpu.VMEM((slots, 2, n, rows, HALF), jnp.bfloat16) for n in blocks]
        + [
            pltpu.VMEM((tiles if stage else ring, 2, n, rows, HALF), jnp.bfloat16)
            for stage, n in enumerate(blocks)
        ]
        + [pltpu.VMEM((n, length, sub_width), jnp.bfloat16) for n in tblocks] * 2
        + [dma((6,)), dma((2, 3)), dma((count - 1,)), dma((count - 1,))]
        + [dma((cbits, tiles, 2)), dma((cbits, tiles, 2))]
        + [dma((tbits, tblocks[0])), dma((tbits, tblocks[0]))]
        + [pltpu.SemaphoreType.REGULAR],
        compiler_params=pltpu.CompilerParams(
            collective_id=call, has_side_effects=True, vmem_limit_bytes=63 * 1024 * 1024
        ),
        cost_estimate=pl.CostEstimate(
            flops=14 * depth * length * columns,
            bytes_accessed=2 * (depth * length + 3 * length * columns + 3 * depth * columns),
            transcendentals=0,
        ),
        name="tail",
    )(upstream, turned, *rows_in, *weights, *summaries, mask, grad_out)


def per_device(tokens, w_query, w_key, w_value, w_out, block_doc, grad_out):
    score_scale_factor = 1.0 / math.sqrt(HDIM)
    tok_rows = tokens.shape[0]
    col_count = w_query.shape[1]
    blocks = tok_rows // BLOCK
    head_count = col_count // HDIM
    block_shape = (blocks, BLOCK, head_count, HDIM)
    upstream = lax.all_gather(grad_out.T, "tp", axis=0, tiled=True)

    def project(weight):
        return jnp.dot(tokens, weight, preferred_element_type=jnp.float32).astype(jnp.bfloat16)

    query, key, value = project(w_query), project(w_key), project(w_value)
    query_row_matrix = query.reshape(block_shape)
    key_row_matrix = key.reshape(block_shape)
    value_row_matrix = value.reshape(block_shape)
    own_key = key_row_matrix[:, BLOCK - 1].reshape(blocks, col_count)
    own_value = value_row_matrix[:, BLOCK - 1].reshape(blocks, col_count)
    summary = lax.all_gather(
        jnp.concatenate([own_key, own_value], axis=1), "ctx", axis=0, tiled=True
    )
    flat_key, flat_value = summary[:, :col_count], summary[:, col_count:]
    total_blocks = summary.shape[0]
    summary_key = flat_key.reshape(total_blocks, head_count, HDIM)
    summary_value = flat_value.reshape(total_blocks, head_count, HDIM)
    first_block = lax.axis_index("ctx") * blocks
    query_ids = first_block + jnp.arange(blocks, dtype=jnp.int32)
    own_doc = lax.dynamic_slice_in_dim(block_doc, first_block, blocks, 0)
    block_ids = jnp.arange(total_blocks, dtype=jnp.int32)
    allowed = (block_ids[None, :] < query_ids[:, None]) & (block_doc[None, :] == own_doc[:, None])
    positions = jnp.arange(BLOCK, dtype=jnp.int32)
    causal = positions[None, :] <= positions[:, None]
    combined_output = attend(
        query_row_matrix,
        key_row_matrix,
        value_row_matrix,
        summary_key,
        summary_value,
        allowed,
        causal,
        score_scale_factor,
    )
    attn = combined_output.reshape(tok_rows, col_count)
    partial_value = jnp.dot(attn, w_out, preferred_element_type=jnp.float32)
    turned = tokens.T
    pieces = column_pieces(partial_value, "tp")
    upstream, pieces, turned = lax.optimization_barrier((upstream, pieces, turned))
    moved = send_pieces(pieces, "tp")
    joined, grad_tokens = tail(
        upstream,
        turned,
        (attn, query, key, value),
        (w_out, w_query, w_key, w_value),
        (flat_key, flat_value),
        allowed,
        grad_out,
        ("ctx", "tp"),
        score_scale_factor,
        0,
    )
    joined, moved = lax.optimization_barrier((joined, moved))
    shard_width = grad_out.shape[1]
    summed = lax.dynamic_slice_in_dim(tokens, lax.axis_index("tp") * shard_width, shard_width, 1)
    summed = summed.astype(jnp.float32) + pieces[0]
    for piece in moved:
        summed = summed + piece.astype(jnp.float32)
    output = summed.astype(jnp.bfloat16)
    return (output, grad_tokens, joined[1], joined[2], joined[3], joined[0].T)


def solution(mesh):
    in_specs = (
        P("ctx", None),
        P(None, "tp"),
        P(None, "tp"),
        P(None, "tp"),
        P("tp", None),
        P(),
        P("ctx", "tp"),
    )
    out_specs = (
        P("ctx", "tp"),
        P("ctx", "tp"),
        P("ctx", "tp"),
        P("ctx", "tp"),
        P("ctx", "tp"),
        P("tp", "ctx"),
    )
    return jax.shard_map(
        per_device, mesh=mesh, in_specs=in_specs, out_specs=out_specs, check_vma=False
    )
```
